32 devices in a mesh: seq: 2 (over x), ctx: 4 (over y, core), exp: 4 (over z).
Axes of the slice: x: 2, y: 2, z: 4, core: 2. Of those that a mesh axis runs over, the one named last changes fastest.
Arguments:
- tokens: bfloat16 [2, 2048, 7168], P('seq', ('ctx', 'exp')), may hold values from -8 to 8
- routing: int32 [2, 2048, 8], P('seq', ('ctx', 'exp')), may hold values from 0 to 255, as said below
- router_weight: bfloat16 [7168, 256], replicated, may hold values from -0.0625 to 0.0625
- w_gate: bfloat16 [8, 7168, 2048], P(('seq', 'exp'), None, 'ctx'), may hold values from -0.0625 to 0.0625
- w_up: bfloat16 [8, 7168, 2048], P(('seq', 'exp'), None, 'ctx'), may hold values from -0.0625 to 0.0625
- w_down: bfloat16 [8, 2048, 7168], P(('seq', 'exp'), 'ctx'), may hold values from -0.125 to 0.125
Outputs:
- routed: bfloat16 [2, 2048, 7168], P('seq', ('ctx', 'exp'))
- balance: float32 [2, 256], P('seq')
The draws below stay inside these ranges and needn't reach their ends.
Inputs may be any that keep to these rules, and one draw needn't show every extreme that they name: `routing`: each token names 8 different experts. The rows of one device name any one expert at least 3 and at most 5 times; in every draw one expert below 8 is named exactly 5 times by the rows of every device.
All inputs are finite; a program needn't handle non-finite values.
Results may differ from the reference program's by a relative error of at most 0.014.
Values may be sent and summed in bfloat16 or wider, within the bound.
A program may use at most 128 MiB of HBM per device.

```python
import jax
import jax.numpy as jnp
from jax import lax

D = 7168
FF = 2048
EXPERTS = 256
TOP = 8
TOK_DEV = 128
FLIGHT = 8
SEQS = 2
LENGTH = 2048
CAPACITY = 5
N_SEQ = 2
N_CTX = 4
N_EXP = 4


def draw_tokens(key, part):
    key_jitter, key_direction = jax.random.split(key, 2)
    positions = jnp.arange(LENGTH, dtype=jnp.float32) / (LENGTH - 1)
    direction = jax.random.normal(key_direction, (SEQS, 1, D), jnp.float32)
    jitter_part = jax.random.normal(key_jitter, (SEQS, LENGTH, D), jnp.float32)
    strength = 0.3 + 0.6 * positions
    values = jitter_part + strength[None, :, None] * direction
    return jnp.clip(values, -8.0, 8.0).astype(jnp.bfloat16)


def draw_routing(key, part):
    blocks = SEQS * LENGTH // TOK_DEV
    classes = EXPERTS // TOP
    mean_load = TOK_DEV * TOP // EXPERTS
    reach = mean_load // 4
    key_pick, key_shift, key_order, key_lift, key_perm = jax.random.split(key, 5)
    full_expert = jax.random.randint(key_pick, (), 0, FLIGHT).astype(jnp.int32)
    shifts = jax.random.randint(key_shift, (blocks, classes // 2), -reach, reach + 1).astype(jnp.int32)
    shifts = shifts.at[:, 0].set(reach)
    counts = jnp.stack([mean_load + shifts, mean_load - shifts], axis=2).reshape(blocks, classes)
    bounds = jnp.cumsum(counts, axis=1).astype(jnp.int32)
    ranks = jnp.arange(TOK_DEV, dtype=jnp.int32)
    class_of_rank = jnp.sum((ranks[None, :, None] >= bounds[:, None, :]).astype(jnp.int32), axis=2).astype(jnp.int32)
    orders = jax.vmap(lambda sub: jax.random.permutation(sub, TOK_DEV))(jax.random.split(key_order, blocks)).astype(jnp.int32)
    token_class = jnp.take_along_axis(class_of_rank, orders, axis=1)
    lifts = jax.random.randint(key_lift, (blocks, TOK_DEV), 0, TOP).astype(jnp.int32)
    base = token_class + classes * lifts
    perms = jax.vmap(lambda sub: jax.random.permutation(sub, EXPERTS))(jax.random.split(key_perm, blocks)).astype(jnp.int32)
    where_full = jnp.argmax(perms == full_expert, axis=1).astype(jnp.int32)
    first_entry = perms[:, 0]
    positions = jnp.arange(EXPERTS, dtype=jnp.int32)[None, :]
    perms = jnp.where(positions == 0, full_expert, jnp.where(positions == where_full[:, None], first_entry[:, None], perms))
    offsets = jnp.arange(TOP, dtype=jnp.int32) * classes
    picks = (base[:, :, None] + offsets[None, None, :]) % EXPERTS
    chosen = jnp.take_along_axis(perms, picks.reshape(blocks, TOK_DEV * TOP), axis=1)
    return chosen.reshape(SEQS, LENGTH, TOP).astype(jnp.int32)


def block_scale(stream_key, dims, cuts, low, top_value):
    def one(position, shards_of):
        steps = jax.random.uniform(jax.random.fold_in(jax.random.fold_in(stream_key, 6), position), (shards_of,), jnp.float32, low / len(cuts), top_value / len(cuts))
        return jnp.repeat(jnp.exp(steps), dims[position] // shards_of).reshape((-1,) + (1,) * (len(dims) - position - 1))

    factor_of = one(*cuts[0])
    for cut in cuts[1:]:
        factor_of = factor_of * one(*cut)
    return factor_of


def scatter_about(stream_key, shape, width, most, shards=(), kind=jnp.bfloat16):
    factor_of = block_scale(stream_key, shape, shards, -0.22, 0.18) if shards else 1.0
    drawn = jax.random.normal(stream_key, shape, jnp.float32) * width * factor_of
    return jnp.minimum(jnp.maximum(drawn, -most), most).astype(kind)


def setup_inputs(seed: int = 0) -> dict:
    splits = jax.random.split(jax.random.key(seed), 7)
    tokens = draw_tokens(jax.random.fold_in(splits[6], 71), 0)
    routing = draw_routing(jax.random.fold_in(splits[6], 71), 0)
    router_weight = scatter_about(splits[2], (D, EXPERTS), D ** -0.5, 0.0625)
    w_gate = scatter_about(splits[3], (FLIGHT, D, FF), D ** -0.5, 0.0625, ((0, 8), (2, 4)))
    w_up = scatter_about(splits[4], (FLIGHT, D, FF), D ** -0.5, 0.0625, ((0, 8), (2, 4)))
    w_down = scatter_about(splits[5], (FLIGHT, FF, D), FF ** -0.5, 0.125, ((0, 8), (1, 4)))
    return dict(tokens=tokens, routing=routing, router_weight=router_weight, w_gate=w_gate, w_up=w_up, w_down=w_down)


route_scale = 2.5


def expert_block(row_block, gate_weight, up_weight, down_weight):
    gate_proj = jnp.dot(row_block, gate_weight, preferred_element_type=jnp.float32)
    up_proj = jnp.dot(row_block, up_weight, preferred_element_type=jnp.float32)
    hidden = (jax.nn.silu(gate_proj) * up_proj).astype(jnp.bfloat16)
    block_width = FF // N_CTX
    combined = jnp.zeros((row_block.shape[0], D), jnp.float32)
    for column in range(N_CTX):
        lower = column * block_width
        partial_value = jnp.dot(hidden[:, lower:lower + block_width], down_weight[lower:lower + block_width], preferred_element_type=jnp.float32)
        rounded = lax.optimization_barrier(partial_value.astype(jnp.bfloat16))
        combined = combined + rounded.astype(jnp.float32)
    return combined.astype(jnp.bfloat16)


def reference(tokens, routing, router_weight, w_gate, w_up, w_down):
    flight = N_SEQ * N_EXP
    blocks = SEQS * LENGTH // TOK_DEV
    per_block = TOK_DEV * TOP
    flat_tokens = tokens.reshape(SEQS * LENGTH, D)
    routes = routing.reshape(SEQS * LENGTH, TOP)
    logits = jnp.dot(flat_tokens, router_weight, preferred_element_type=jnp.float32)
    scores = jax.nn.sigmoid(logits)
    affinity = scores / jnp.sum(scores, axis=1, keepdims=True)
    picked = jnp.take_along_axis(scores, routes, axis=1)
    gate_weights = picked / jnp.sum(picked, axis=1, keepdims=True) * route_scale
    prob_sum = jnp.sum(affinity.reshape(SEQS, LENGTH, EXPERTS), axis=1)
    seq_of_row = (jnp.arange(SEQS * LENGTH, dtype=jnp.int32) // LENGTH)[:, None]
    load = jnp.zeros((SEQS, EXPERTS), jnp.float32).at[jnp.broadcast_to(seq_of_row, routes.shape), routes].add(1.0)
    balance = load * (EXPERTS / (TOP * LENGTH)) * (prob_sum / LENGTH) * EXPERTS

    block_routes = routes.reshape(blocks, per_block)
    expert_iota = jnp.arange(flight, dtype=jnp.int32)[None, None, :]
    onehot = (block_routes[:, :, None] == expert_iota).astype(jnp.int32)
    slot_rank = jnp.sum((jnp.cumsum(onehot, axis=1) - onehot) * onehot, axis=2)
    is_live = block_routes < flight
    block_ids = jnp.arange(blocks, dtype=jnp.int32)[:, None]
    row_index = block_routes * (blocks * CAPACITY) + block_ids * CAPACITY + slot_rank
    spare = flight * blocks * CAPACITY
    target = jnp.where(is_live, row_index, spare)
    owner = block_ids * TOK_DEV + jnp.arange(per_block, dtype=jnp.int32)[None, :] // TOP
    source_row = jnp.zeros((spare + 1,), jnp.int32).at[target.reshape(-1)].set(owner.reshape(-1))
    filled = jnp.zeros((spare + 1,), jnp.int32).at[target.reshape(-1)].set(1)
    source_row = source_row[:spare].reshape(flight, blocks * CAPACITY)
    filled = filled[:spare].reshape(flight, blocks * CAPACITY)

    def one_expert(inputs):
        rows_of, filled_of, gate_weight, up_weight, down_weight = inputs
        row_block = jnp.where(filled_of[:, None] > 0, flat_tokens[rows_of], jnp.zeros((), flat_tokens.dtype))
        return expert_block(row_block, gate_weight, up_weight, down_weight)

    expert_out = lax.map(one_expert, (source_row, filled, w_gate, w_up, w_down))
    expert_out = expert_out.reshape(spare, D)
    live_gates = jnp.where(is_live, gate_weights.reshape(blocks, per_block), 0.0).reshape(SEQS * LENGTH, TOP)
    gather_index = jnp.where(is_live, row_index, 0).reshape(SEQS * LENGTH, TOP)
    combined = jnp.zeros((SEQS * LENGTH, D), jnp.float32)
    for column in range(TOP):
        combined = combined + live_gates[:, column:column + 1] * expert_out[gather_index[:, column]]
    routed = combined.astype(jnp.bfloat16).reshape(SEQS, LENGTH, D)
    return routed, balance
```

```python
import functools

import jax
import jax.numpy as jnp
from jax import lax
from jax.experimental import pallas as pl
from jax.experimental.pallas import tpu as pltpu
from jax.sharding import PartitionSpec as P

route_scale = 2.5
LANES = 128
SUBS = 8
MESH = pl.DeviceIdType.MESH
f32 = jnp.float32
bf16 = jnp.bfloat16


def dot(a, b):
    return jnp.dot(a, b, preferred_element_type=f32)


def pack(rows, cap):
    sub = lax.broadcasted_iota(jnp.int32, (1, SUBS, LANES), 1)
    pieces = []
    for q in range(cap):
        piece = rows[:, :, q * LANES : (q + 1) * LANES]
        for s in range(cap, SUBS):
            piece = jnp.where(sub == s, rows[:, q : q + 1, s * LANES : (s + 1) * LANES], piece)
        pieces.append(piece)
    return jnp.concatenate(pieces, axis=2)


def unpack(dense, cap):
    sub = lax.broadcasted_iota(jnp.int32, (1, SUBS, LANES), 1)
    pieces = []
    for b in range(SUBS):
        if b < cap:
            piece = dense[:, :, b * LANES : (b + 1) * LANES]
        else:
            piece = jnp.broadcast_to(dense[:, b : b + 1, 0:LANES], dense.shape[:2] + (LANES,))
            for r in range(1, cap):
                piece = jnp.where(sub == r, dense[:, b : b + 1, r * LANES : (r + 1) * LANES], piece)
        pieces.append(piece)
    return jnp.concatenate(pieces, axis=2)


def kernel(
    cfg,
    tokens, routes, routes_t, router_weight, w_gate, w_up, w_down,
    out, bal,
    tok, rw, wg, wu, wd, outv,
    mout, minn, xs, acc, sel_s, gates, hid,
    ps, pr, keep, ys, yr, ykeep, rout, rin, stat,
    tok_sem, rw_sem, wg_sem, wu_sem, wd_sem, out_sem,
    d_send, d_recv, y_send, y_recv, c_send, c_recv,
    p_send, p_recv, v_send, v_recv, r_send, r_recv, s_send, s_recv,
):
    (steps, width, cap, flight, n_seq, n_ctx, n_exp, n_tok, top, experts) = cfg
    n_y = n_ctx // 2
    slots = flight * SUBS
    rows = flight * cap
    length = n_tok * n_ctx * n_exp
    seq, ctx, exp = lax.axis_index("seq"), lax.axis_index("ctx"), lax.axis_index("exp")
    me = seq * n_exp + exp
    my_y, core = ctx // 2, ctx % 2

    def group(o):
        p = (me + o) % flight
        return p, (p // n_exp, ctx, p % n_exp)

    def y_peer(o):
        y = (my_y + o) % n_y
        return y, (seq, y * 2 + core, exp)

    partner = (seq, ctx + 1 - 2 * core, exp)

    barrier = pltpu.get_barrier_semaphore()
    for o in range(1, flight):
        pl.semaphore_signal(barrier, inc=1, device_id=group(o)[1], device_id_type=MESH)
    for o in range(1, n_ctx):
        pl.semaphore_signal(barrier, inc=1, device_id=(seq, (ctx + o) % n_ctx, exp), device_id_type=MESH)

    def local(c, which):
        cols = pl.ds(pl.multiple_of(c * width, width), width)
        src, dst, sem = (
            lambda: (tokens.at[0, :, cols], tok.at[c], tok_sem.at[c]),
            lambda: (router_weight.at[cols], rw.at[c], rw_sem.at[c]),
            lambda: (w_gate.at[0, cols], wg.at[c], wg_sem.at[c]),
            lambda: (w_up.at[0, cols], wu.at[c], wu_sem.at[c]),
            lambda: (w_down.at[0, :, cols], wd.at[c], wd_sem.at[c]),
            lambda: (outv.at[c], out.at[0, :, cols], out_sem.at[c]),
        )[which]()
        return pltpu.make_async_copy(src, dst, sem)

    for which in range(5):
        @pl.loop(0, steps)
        def _(c):
            local(c, which).start()

    rt = routes_t[...]
    slot_expert = lax.broadcasted_iota(jnp.int32, (slots, n_tok), 0)
    hit_t = jnp.zeros((slots, n_tok), f32)
    for k in range(top):
        hit_t = hit_t + (rt[k : k + 1, :] == slot_expert // SUBS).astype(f32)
    ti = lax.broadcasted_iota(jnp.int32, (n_tok, n_tok), 0)
    tj = lax.broadcasted_iota(jnp.int32, (n_tok, n_tok), 1)
    rank_t = dot(hit_t.astype(bf16), (ti < tj).astype(f32).astype(bf16))
    pick_t = jnp.where(rank_t == (slot_expert % SUBS).astype(f32), hit_t, 0.0)
    sel_s[...] = pick_t.astype(bf16)

    def dispatch(c, o):
        p, dev = group(o)
        return pltpu.make_async_remote_copy(
            src_ref=mout.at[c, p], dst_ref=minn.at[c, me], send_sem=d_send.at[c, o], recv_sem=d_recv.at[c, o],
            device_id=dev, device_id_type=MESH)

    def spread(c, o):
        _, dev = y_peer(o)
        return pltpu.make_async_remote_copy(
            src_ref=xs.at[c, ctx], dst_ref=xs.at[c, ctx], send_sem=y_send.at[c, o], recv_sem=y_recv.at[c, o],
            device_id=dev, device_id_type=MESH)

    def hand(c, o):
        y = (my_y + o) % n_y
        slot = y * 2 + core
        return pltpu.make_async_remote_copy(
            src_ref=xs.at[c, slot], dst_ref=xs.at[c, slot], send_sem=c_send.at[c, o], recv_sem=c_recv.at[c, o],
            device_id=partner, device_id_type=MESH)

    pl.semaphore_wait(barrier, flight - 1 + n_ctx - 1)

    @pl.loop(0, steps)
    def _(c):
        local(c, 0).wait()
        picked = dot(sel_s[...], tok[c]).reshape(flight, SUBS, width)
        mout[c] = pack(picked, cap).astype(bf16)
        minn[c, me] = mout[c, me]
        for o in range(1, flight):
            dispatch(c, o).start()

    acc_r = jnp.zeros((n_tok, experts), f32)

    def route_step(c, total):
        local(c, 1).wait()
        return total + dot(tok[c], rw[c])

    logits = lax.fori_loop(0, steps, route_step, acc_r)
    scores = jax.nn.sigmoid(logits)
    affinity = scores / jnp.sum(scores, axis=1, keepdims=True)
    rr = routes[0]
    lane = lax.broadcasted_iota(jnp.int32, (n_tok, experts), 1)
    hit = jnp.zeros((n_tok, experts), f32)
    for k in range(top):
        hit = hit + (rr[:, k : k + 1] == lane).astype(f32)
    gate = hit * scores / jnp.sum(hit * scores, axis=1, keepdims=True) * route_scale
    stat[ctx, 0:1] = jnp.sum(affinity, axis=0, keepdims=True)
    stat[ctx, 1:2] = jnp.sum(hit, axis=0, keepdims=True)

    def stat_ctx(o):
        return pltpu.make_async_remote_copy(
            src_ref=stat.at[ctx], dst_ref=stat.at[ctx], send_sem=s_send.at[o], recv_sem=s_recv.at[o],
            device_id=(seq, (ctx + o) % n_ctx, exp), device_id_type=MESH)

    def stat_exp(o):
        slot = n_ctx + exp
        return pltpu.make_async_remote_copy(
            src_ref=stat.at[slot], dst_ref=stat.at[slot], send_sem=s_send.at[n_ctx + o],
            recv_sem=s_recv.at[n_ctx + o], device_id=(seq, ctx, (exp + o) % n_exp), device_id_type=MESH)

    for o in range(1, n_ctx):
        stat_ctx(o).start()

    rank = dot((ti > tj).astype(f32).astype(bf16), hit.astype(bf16))
    ei = lax.broadcasted_iota(jnp.int32, (experts, slots), 0)
    ej = lax.broadcasted_iota(jnp.int32, (experts, slots), 1)
    widen = (ei == ej // SUBS).astype(f32).astype(bf16)
    place = (lax.broadcasted_iota(jnp.int32, (n_tok, slots), 1) % SUBS).astype(f32)
    here = dot(rank.astype(bf16), widen) == place
    high = gate.astype(bf16)
    low = (gate - high.astype(f32)).astype(bf16)
    gates[0] = jnp.where(here, dot(high, widen), 0.0).astype(bf16)
    gates[1] = jnp.where(here, dot(low, widen), 0.0).astype(bf16)

    ri = lax.broadcasted_iota(jnp.int32, (rows, slots), 0)
    rj = lax.broadcasted_iota(jnp.int32, (rows, slots), 1)
    squeeze = ((ri // cap == rj // SUBS) & (ri % cap == rj % SUBS)).astype(f32).astype(bf16)
    si = lax.broadcasted_iota(jnp.int32, (slots, rows), 0)
    sj = lax.broadcasted_iota(jnp.int32, (slots, rows), 1)
    expand = ((sj // cap == si // SUBS) & (sj % cap == si % SUBS)).astype(f32).astype(bf16)

    acc[...] = jnp.zeros_like(acc)

    @pl.loop(0, steps + 2)
    def _(i):
        @pl.when(i < steps)
        def _():
            c = i
            for o in range(1, flight):
                dispatch(c, o).wait_recv()
            loose = unpack(minn[c].astype(f32), cap).reshape(slots, width).astype(bf16)
            xs[c, ctx] = dot(squeeze, loose).astype(bf16)
            for o in range(1, n_y):
                spread(c, o).start()
            hand(c, 0).start()

        @pl.when((i >= 1) & (i < steps + 1))
        def _():
            c = i - 1
            for o in range(1, n_y):
                spread(c, n_y - o).wait_recv()
                hand(c, o).start()

        @pl.when(i >= 2)
        def _():
            c = i - 2
            for o in range(n_y):
                hand(c, o).wait_recv()
            x = jnp.concatenate([xs[c, j].astype(f32) for j in range(n_ctx)], axis=0).astype(bf16)
            local(c, 2).wait()
            local(c, 3).wait()
            acc[0] += dot(x, wg[c])
            acc[1] += dot(x, wu[c])

    gv = acc[0]
    hid[...] = (gv / (1.0 + jnp.exp(-gv)) * acc[1]).astype(bf16)

    for o in range(1, n_ctx):
        stat_ctx(o).wait_recv()
    ctx_total = stat[0]
    for j in range(1, n_ctx):
        ctx_total = ctx_total + stat[j]
    stat[n_ctx + exp] = ctx_total
    for o in range(1, n_exp):
        stat_exp(o).start()

    def pair(c):
        return pltpu.make_async_remote_copy(
            src_ref=ps.at[c], dst_ref=pr.at[c], send_sem=p_send.at[c], recv_sem=p_recv.at[c],
            device_id=partner, device_id_type=MESH)

    def back_y(c, o):
        y, dev = y_peer(o)
        return pltpu.make_async_remote_copy(
            src_ref=ys.at[c, o], dst_ref=yr.at[c, o], send_sem=v_send.at[c, o], recv_sem=v_recv.at[c, o],
            device_id=dev, device_id_type=MESH)

    def back(c, o):
        p, dev = group(o)
        return pltpu.make_async_remote_copy(
            src_ref=rout.at[c, p], dst_ref=rin.at[c, me], send_sem=r_send.at[c, o], recv_sem=r_recv.at[c, o],
            device_id=dev, device_id_type=MESH)

    @pl.loop(0, steps + 3)
    def _(i):
        @pl.when(i < steps)
        def _():
            c = i
            local(c, 4).wait()
            part = dot(hid[...], wd[c])
            for y in range(n_y):
                a = part[(2 * y) * rows : (2 * y + 1) * rows]
                b = part[(2 * y + 1) * rows : (2 * y + 2) * rows]
                ps[c, y] = jnp.where(core == 0, b, a).astype(bf16)
                keep[c, y] = jnp.where(core == 0, a, b).astype(bf16)
            pair(c).start()

        @pl.when((i >= 1) & (i < steps + 1))
        def _():
            c = i - 1
            pair(c).wait_recv()
            for o in range(n_y):
                y = (my_y + o) % n_y
                both = keep[c, y].astype(f32) + pr[c, y].astype(f32)
                if o == 0:
                    ykeep[c] = both
                else:
                    ys[c, o] = both.astype(bf16)
                    back_y(c, o).start()

        @pl.when((i >= 2) & (i < steps + 2))
        def _():
            c = i - 2
            total = ykeep[c]
            for o in range(1, n_y):
                back_y(c, o).wait_recv()
                total = total + yr[c, o].astype(f32)
            spaced = dot(expand, total.astype(bf16)).reshape(flight, SUBS, width)
            rout[c] = pack(spaced, cap).astype(bf16)
            rin[c, me] = rout[c, me]
            for o in range(1, flight):
                back(c, o).start()

        @pl.when(i >= 3)
        def _():
            c = i - 3
            for o in range(1, flight):
                back(c, o).wait_recv()
            got = unpack(rin[c].astype(f32), cap).reshape(slots, width).astype(bf16)
            outv[c] = (dot(gates[0], got) + dot(gates[1], got)).astype(bf16)
            local(c, 5).start()

    for o in range(1, n_exp):
        stat_exp(o).wait_recv()
    total = stat[n_ctx]
    for j in range(1, n_exp):
        total = total + stat[n_ctx + j]
    bal[...] = total[1:2] * (experts / (top * length)) * (total[0:1] / length) * experts

    for o in range(1, n_ctx):
        stat_ctx(o).wait_send()
    for o in range(1, n_exp):
        stat_exp(o).wait_send()

    @pl.loop(0, steps)
    def _(c):
        for o in range(1, flight):
            dispatch(c, o).wait_send()
            back(c, o).wait_send()
        for o in range(1, n_y):
            spread(c, o).wait_send()
            back_y(c, o).wait_send()
        for o in range(n_y):
            hand(c, o).wait_send()
        pair(c).wait_send()
        local(c, 5).wait()


def on_device(tokens, routing, router_weight, w_gate, w_up, w_down):
    n_seq, n_ctx, n_exp = (lax.axis_size(a) for a in ("seq", "ctx", "exp"))
    _, n_tok, features = tokens.shape
    top = routing.shape[2]
    experts = router_weight.shape[1]
    ff = w_gate.shape[2]
    flight = n_seq * n_exp
    mean_load = n_tok * top // experts
    cap = mean_load + mean_load // 4
    width = SUBS * LANES
    steps = features // width
    n_y = n_ctx // 2
    rows = flight * cap
    slots = flight * SUBS
    cfg = (steps, width, cap, flight, n_seq, n_ctx, n_exp, n_tok, top, experts)
    V = pltpu.VMEM
    dma = pltpu.SemaphoreType.DMA
    dense = cap * LANES
    scratch = [
        V((steps, n_tok, width), bf16), V((steps, width, experts), bf16), V((steps, width, ff), bf16),
        V((steps, width, ff), bf16), V((steps, ff, width), bf16), V((steps, n_tok, width), bf16),
        V((steps, flight, SUBS, dense), bf16), V((steps, flight, SUBS, dense), bf16),
        V((steps, n_ctx, rows, width), bf16), V((2, n_ctx * rows, ff), f32), V((slots, n_tok), bf16),
        V((2, n_tok, slots), bf16), V((n_ctx * rows, ff), bf16),
        V((steps, n_y, rows, width), bf16), V((steps, n_y, rows, width), bf16), V((steps, n_y, rows, width), bf16),
        V((steps, n_y, rows, width), bf16), V((steps, n_y, rows, width), bf16), V((steps, rows, width), f32),
        V((steps, flight, SUBS, dense), bf16), V((steps, flight, SUBS, dense), bf16),
        V((n_ctx + n_exp, 2, experts), f32),
    ]
    scratch += [dma((steps,)) for _ in range(6)]
    scratch += [dma((steps, flight)), dma((steps, flight)), dma((steps, n_y)), dma((steps, n_y)),
                dma((steps, n_y)), dma((steps, n_y)), dma((steps,)), dma((steps,)),
                dma((steps, n_y)), dma((steps, n_y)), dma((steps, flight)), dma((steps, flight)),
                dma((n_ctx + n_exp,)), dma((n_ctx + n_exp,))]
    hbm = pl.BlockSpec(memory_space=pl.ANY)
    vm = pl.BlockSpec(memory_space=pltpu.VMEM)
    return pl.pallas_call(
        functools.partial(kernel, cfg),
        out_shape=(jax.ShapeDtypeStruct(tokens.shape, bf16), jax.ShapeDtypeStruct((1, experts), f32)),
        in_specs=[hbm, vm, vm, hbm, hbm, hbm, hbm],
        out_specs=(hbm, vm),
        scratch_shapes=scratch,
        compiler_params=pltpu.CompilerParams(
            collective_id=0, has_side_effects=True, vmem_limit_bytes=60 * 1024 * 1024),
    )(tokens, routing, routing[0].T, router_weight, w_gate, w_up, w_down)


def solution(mesh):
    placed = (
        P("seq", ("ctx", "exp"), None),
        P("seq", ("ctx", "exp"), None),
        P(),
        P(("seq", "exp"), None, "ctx"),
        P(("seq", "exp"), None, "ctx"),
        P(("seq", "exp"), "ctx", None),
    )
    return jax.shard_map(
        on_device,
        mesh=mesh,
        in_specs=placed,
        out_specs=(P("seq", ("ctx", "exp"), None), P("seq", None)),
        check_vma=False,
    )
```

```python
import functools

import jax
import jax.numpy as jnp
from jax import lax
from jax.experimental import pallas as pl
from jax.experimental.pallas import tpu as pltpu
from jax.sharding import PartitionSpec as P

route_scale = 2.5
LANES = 128
SUBS = 8
MESH = pl.DeviceIdType.MESH
f32 = jnp.float32
bf16 = jnp.bfloat16


def dot(a, b):
    return jnp.dot(a, b, preferred_element_type=f32)


def pack(rows, cap):
    sub = lax.broadcasted_iota(jnp.int32, (1, SUBS, LANES), 1)
    pieces = []
    for q in range(cap):
        piece = rows[:, :, q * LANES : (q + 1) * LANES]
        for s in range(cap, SUBS):
            piece = jnp.where(sub == s, rows[:, q : q + 1, s * LANES : (s + 1) * LANES], piece)
        pieces.append(piece)
    return jnp.concatenate(pieces, axis=2)


def unpack(dense, cap):
    sub = lax.broadcasted_iota(jnp.int32, (1, SUBS, LANES), 1)
    pieces = []
    for b in range(SUBS):
        if b < cap:
            piece = dense[:, :, b * LANES : (b + 1) * LANES]
        else:
            piece = jnp.broadcast_to(dense[:, b : b + 1, 0:LANES], dense.shape[:2] + (LANES,))
            for r in range(1, cap):
                piece = jnp.where(sub == r, dense[:, b : b + 1, r * LANES : (r + 1) * LANES], piece)
        pieces.append(piece)
    return jnp.concatenate(pieces, axis=2)


def kernel(
    cfg,
    tokens, routes_t, router_weight, w_gate, w_up, w_down,
    out, bal,
    tok, rw, wg, wu, wd, outv,
    mout, minn, xs, acc, logits, sel_s, gates, hid,
    ps, pr, keep, ys, yr, ykeep, rout, rin, stat,
    tok_sem, rw_sem, wg_sem, wu_sem, wd_sem, out_sem,
    d_send, d_recv, y_send, y_recv, c_send, c_recv,
    p_send, p_recv, v_send, v_recv, r_send, r_recv, s_send, s_recv,
):
    (steps, width, cap, flight, n_seq, n_ctx, n_exp, n_tok, top, experts) = cfg
    n_y = n_ctx // 2
    slots = flight * SUBS
    rows = flight * cap
    length = n_tok * n_ctx * n_exp
    seq, ctx, exp = lax.axis_index("seq"), lax.axis_index("ctx"), lax.axis_index("exp")
    me = seq * n_exp + exp
    my_y, core = ctx // 2, ctx % 2

    def group(o):
        p = (me + o) % flight
        return p, (p // n_exp, ctx, p % n_exp)

    def y_peer(o):
        y = (my_y + o) % n_y
        return y, (seq, y * 2 + core, exp)

    partner = (seq, ctx + 1 - 2 * core, exp)

    barrier = pltpu.get_barrier_semaphore()
    for o in range(1, flight):
        pl.semaphore_signal(barrier, inc=1, device_id=group(o)[1], device_id_type=MESH)
    for o in range(1, n_ctx):
        pl.semaphore_signal(barrier, inc=1, device_id=(seq, (ctx + o) % n_ctx, exp), device_id_type=MESH)

    def local(c, which):
        cols = pl.ds(pl.multiple_of(c * width, width), width)
        src, dst, sem = (
            lambda: (tokens.at[0, :, cols], tok.at[c], tok_sem.at[c]),
            lambda: (router_weight.at[cols], rw.at[c], rw_sem.at[c]),
            lambda: (w_gate.at[0, cols], wg.at[c], wg_sem.at[c]),
            lambda: (w_up.at[0, cols], wu.at[c], wu_sem.at[c]),
            lambda: (w_down.at[0, :, cols], wd.at[c], wd_sem.at[c]),
            lambda: (outv.at[c], out.at[0, :, cols], out_sem.at[c]),
        )[which]()
        return pltpu.make_async_copy(src, dst, sem)

    @pl.loop(0, steps)
    def _(c):
        local(c, 0).start()

    rt = routes_t[...]
    slot_expert = lax.broadcasted_iota(jnp.int32, (slots, n_tok), 0)
    hit_t = jnp.zeros((slots, n_tok), f32)
    for k in range(top):
        hit_t = hit_t + (rt[k : k + 1, :] == slot_expert // SUBS).astype(f32)
    ti = lax.broadcasted_iota(jnp.int32, (n_tok, n_tok), 0)
    tj = lax.broadcasted_iota(jnp.int32, (n_tok, n_tok), 1)
    rank_t = dot(hit_t.astype(bf16), (ti < tj).astype(f32).astype(bf16))
    pick_t = jnp.where(rank_t == (slot_expert % SUBS).astype(f32), hit_t, 0.0)
    sel_s[...] = pick_t.astype(bf16)

    def dispatch(c, o):
        p, dev = group(o)
        return pltpu.make_async_remote_copy(
            src_ref=mout.at[c, p], dst_ref=minn.at[c, me], send_sem=d_send.at[c, o], recv_sem=d_recv.at[c, o],
            device_id=dev, device_id_type=MESH)

    def spread(c, o):
        _, dev = y_peer(o)
        return pltpu.make_async_remote_copy(
            src_ref=xs.at[c, ctx], dst_ref=xs.at[c, ctx], send_sem=y_send.at[c, o], recv_sem=y_recv.at[c, o],
            device_id=dev, device_id_type=MESH)

    def hand(c, o):
        y = (my_y + o) % n_y
        slot = y * 2 + core
        return pltpu.make_async_remote_copy(
            src_ref=xs.at[c, slot], dst_ref=xs.at[c, slot], send_sem=c_send.at[c, o], recv_sem=c_recv.at[c, o],
            device_id=partner, device_id_type=MESH)

    pl.semaphore_wait(barrier, flight - 1 + n_ctx - 1)

    @pl.loop(0, steps)
    def _(c):
        local(c, 0).wait()
        picked = dot(sel_s[...], tok[c]).reshape(flight, SUBS, width)
        mout[c] = pack(picked, cap).astype(bf16)
        minn[c, me] = mout[c, me]
        for o in range(1, flight):
            dispatch(c, o).start()
        for which in range(1, 4):
            local(c, which).start()

    @pl.loop(0, steps)
    def _(c):
        local(c, 4).start()

    def stat_ctx(o):
        return pltpu.make_async_remote_copy(
            src_ref=stat.at[ctx], dst_ref=stat.at[ctx], send_sem=s_send.at[o], recv_sem=s_recv.at[o],
            device_id=(seq, (ctx + o) % n_ctx, exp), device_id_type=MESH)

    def stat_exp(o):
        slot = n_ctx + exp
        return pltpu.make_async_remote_copy(
            src_ref=stat.at[slot], dst_ref=stat.at[slot], send_sem=s_send.at[n_ctx + o],
            recv_sem=s_recv.at[n_ctx + o], device_id=(seq, ctx, (exp + o) % n_exp), device_id_type=MESH)

    def weigh():
        scores = jax.nn.sigmoid(logits[...])
        affinity = scores / jnp.sum(scores, axis=1, keepdims=True)
        spare = jnp.zeros((n_tok - top, n_tok), f32)
        rr = jnp.concatenate([routes_t[...].astype(f32), spare], axis=0).T
        lane = lax.broadcasted_iota(jnp.int32, (n_tok, experts), 1).astype(f32)
        hit = jnp.zeros((n_tok, experts), f32)
        for k in range(top):
            hit = hit + (rr[:, k : k + 1] == lane).astype(f32)
        gate = hit * scores / jnp.sum(hit * scores, axis=1, keepdims=True) * route_scale
        stat[ctx, 0:1] = jnp.sum(affinity, axis=0, keepdims=True)
        stat[ctx, 1:2] = jnp.sum(hit, axis=0, keepdims=True)
        for o in range(1, n_ctx):
            stat_ctx(o).start()
        rank = dot((ti > tj).astype(f32).astype(bf16), hit.astype(bf16))
        ei = lax.broadcasted_iota(jnp.int32, (experts, slots), 0)
        ej = lax.broadcasted_iota(jnp.int32, (experts, slots), 1)
        widen = (ei == ej // SUBS).astype(f32).astype(bf16)
        place = (lax.broadcasted_iota(jnp.int32, (n_tok, slots), 1) % SUBS).astype(f32)
        here = dot(rank.astype(bf16), widen) == place
        high = gate.astype(bf16)
        low = (gate - high.astype(f32)).astype(bf16)
        gates[0] = jnp.where(here, dot(high, widen), 0.0).astype(bf16)
        gates[1] = jnp.where(here, dot(low, widen), 0.0).astype(bf16)

    def share():
        for o in range(1, n_ctx):
            stat_ctx(o).wait_recv()
        ctx_total = stat[0]
        for j in range(1, n_ctx):
            ctx_total = ctx_total + stat[j]
        stat[n_ctx + exp] = ctx_total
        for o in range(1, n_exp):
            stat_exp(o).start()

    ri = lax.broadcasted_iota(jnp.int32, (rows, slots), 0)
    rj = lax.broadcasted_iota(jnp.int32, (rows, slots), 1)
    squeeze = ((ri // cap == rj // SUBS) & (ri % cap == rj % SUBS)).astype(f32).astype(bf16)
    si = lax.broadcasted_iota(jnp.int32, (slots, rows), 0)
    sj = lax.broadcasted_iota(jnp.int32, (slots, rows), 1)
    expand = ((sj // cap == si // SUBS) & (sj % cap == si % SUBS)).astype(f32).astype(bf16)

    acc[...] = jnp.zeros_like(acc)
    logits[...] = jnp.zeros_like(logits)
    lag_c, lag_d = 2, 3
    lag_f, lag_g, lag_h = 1, 4, 7

    @pl.loop(0, steps + lag_d)
    def _(i):
        @pl.when(i < steps)
        def _():
            c = i
            for o in range(1, flight):
                dispatch(c, o).wait_recv()
            loose = unpack(minn[c].astype(f32), cap).reshape(slots, width).astype(bf16)
            xs[c, ctx] = dot(squeeze, loose).astype(bf16)
            for o in range(1, n_y):
                spread(c, o).start()
            hand(c, 0).start()
            local(c, 1).wait()
            logits[...] += dot(tok[c], rw[c])

        @pl.when((i >= lag_c) & (i < steps + lag_c))
        def _():
            c = i - lag_c
            for o in range(1, n_y):
                spread(c, n_y - o).wait_recv()
                hand(c, o).start()

        @pl.when(i >= lag_d)
        def _():
            c = i - lag_d
            for o in range(n_y):
                hand(c, o).wait_recv()
            x = jnp.concatenate([xs[c, j].astype(f32) for j in range(n_ctx)], axis=0).astype(bf16)
            local(c, 2).wait()
            local(c, 3).wait()
            acc[0] += dot(x, wg[c])
            acc[1] += dot(x, wu[c])

    gv = acc[0]
    hid[...] = (gv / (1.0 + jnp.exp(-gv)) * acc[1]).astype(bf16)

    def pair(c):
        return pltpu.make_async_remote_copy(
            src_ref=ps.at[c], dst_ref=pr.at[c], send_sem=p_send.at[c], recv_sem=p_recv.at[c],
            device_id=partner, device_id_type=MESH)

    def back_y(c, o):
        y, dev = y_peer(o)
        return pltpu.make_async_remote_copy(
            src_ref=ys.at[c, o], dst_ref=yr.at[c, o], send_sem=v_send.at[c, o], recv_sem=v_recv.at[c, o],
            device_id=dev, device_id_type=MESH)

    def back(c, o):
        p, dev = group(o)
        return pltpu.make_async_remote_copy(
            src_ref=rout.at[c, p], dst_ref=rin.at[c, me], send_sem=r_send.at[c, o], recv_sem=r_recv.at[c, o],
            device_id=dev, device_id_type=MESH)

    @pl.loop(0, steps + lag_h)
    def _(i):
        @pl.when(i < steps)
        def _():
            c = i
            local(c, 4).wait()
            part = dot(hid[...], wd[c])
            for y in range(n_y):
                a = part[(2 * y) * rows : (2 * y + 1) * rows]
                b = part[(2 * y + 1) * rows : (2 * y + 2) * rows]
                ps[c, y] = jnp.where(core == 0, b, a).astype(bf16)
                keep[c, y] = jnp.where(core == 0, a, b).astype(bf16)
            pair(c).start()

        @pl.when((i >= lag_f) & (i < steps + lag_f))
        def _():
            c = i - lag_f
            pair(c).wait_recv()
            for o in range(n_y):
                y = (my_y + o) % n_y
                both = keep[c, y].astype(f32) + pr[c, y].astype(f32)
                if o == 0:
                    ykeep[c] = both
                else:
                    ys[c, o] = both.astype(bf16)
                    back_y(c, o).start()

        @pl.when(i == lag_g - 1)
        def _():
            weigh()

        @pl.when(i == lag_h - 1)
        def _():
            share()

        @pl.when((i >= lag_g) & (i < steps + lag_g))
        def _():
            c = i - lag_g
            total = ykeep[c]
            for o in range(1, n_y):
                back_y(c, o).wait_recv()
                total = total + yr[c, o].astype(f32)
            spaced = dot(expand, total.astype(bf16)).reshape(flight, SUBS, width)
            rout[c] = pack(spaced, cap).astype(bf16)
            rin[c, me] = rout[c, me]
            for o in range(1, flight):
                back(c, o).start()

        @pl.when(i >= lag_h)
        def _():
            c = i - lag_h
            for o in range(1, flight):
                back(c, o).wait_recv()
            got = unpack(rin[c].astype(f32), cap).reshape(slots, width).astype(bf16)
            outv[c] = (dot(gates[0], got) + dot(gates[1], got)).astype(bf16)
            local(c, 5).start()

    for o in range(1, n_exp):
        stat_exp(o).wait_recv()
    total = stat[n_ctx]
    for j in range(1, n_exp):
        total = total + stat[n_ctx + j]
    bal[...] = total[1:2] * (experts / (top * length)) * (total[0:1] / length) * experts

    for o in range(1, n_ctx):
        stat_ctx(o).wait_send()
    for o in range(1, n_exp):
        stat_exp(o).wait_send()

    @pl.loop(0, steps)
    def _(c):
        for o in range(1, flight):
            dispatch(c, o).wait_send()
            back(c, o).wait_send()
        for o in range(1, n_y):
            spread(c, o).wait_send()
            back_y(c, o).wait_send()
        for o in range(n_y):
            hand(c, o).wait_send()
        pair(c).wait_send()
        local(c, 5).wait()


def on_device(tokens, routing, router_weight, w_gate, w_up, w_down):
    n_seq, n_ctx, n_exp = (lax.axis_size(a) for a in ("seq", "ctx", "exp"))
    _, n_tok, features = tokens.shape
    top = routing.shape[2]
    experts = router_weight.shape[1]
    ff = w_gate.shape[2]
    flight = n_seq * n_exp
    mean_load = n_tok * top // experts
    cap = mean_load + mean_load // 4
    width = SUBS * LANES
    steps = features // width
    n_y = n_ctx // 2
    rows = flight * cap
    slots = flight * SUBS
    cfg = (steps, width, cap, flight, n_seq, n_ctx, n_exp, n_tok, top, experts)
    V = pltpu.VMEM
    dma = pltpu.SemaphoreType.DMA
    dense = cap * LANES
    scratch = [
        V((steps, n_tok, width), bf16), V((steps, width, experts), bf16), V((steps, width, ff), bf16),
        V((steps, width, ff), bf16), V((steps, ff, width), bf16), V((steps, n_tok, width), bf16),
        V((steps, flight, SUBS, dense), bf16), V((steps, flight, SUBS, dense), bf16),
        V((steps, n_ctx, rows, width), bf16), V((2, n_ctx * rows, ff), f32), V((n_tok, experts), f32),
        V((slots, n_tok), bf16),
        V((2, n_tok, slots), bf16), V((n_ctx * rows, ff), bf16),
        V((steps, n_y, rows, width), bf16), V((steps, n_y, rows, width), bf16), V((steps, n_y, rows, width), bf16),
        V((steps, n_y, rows, width), bf16), V((steps, n_y, rows, width), bf16), V((steps, rows, width), f32),
        V((steps, flight, SUBS, dense), bf16), V((steps, flight, SUBS, dense), bf16),
        V((n_ctx + n_exp, 2, experts), f32),
    ]
    scratch += [dma((steps,)) for _ in range(6)]
    scratch += [dma((steps, flight)), dma((steps, flight)), dma((steps, n_y)), dma((steps, n_y)),
                dma((steps, n_y)), dma((steps, n_y)), dma((steps,)), dma((steps,)),
                dma((steps, n_y)), dma((steps, n_y)), dma((steps, flight)), dma((steps, flight)),
                dma((n_ctx + n_exp,)), dma((n_ctx + n_exp,))]
    hbm = pl.BlockSpec(memory_space=pl.ANY)
    vm = pl.BlockSpec(memory_space=pltpu.VMEM)
    return pl.pallas_call(
        functools.partial(kernel, cfg),
        out_shape=(jax.ShapeDtypeStruct(tokens.shape, bf16), jax.ShapeDtypeStruct((1, experts), f32)),
        in_specs=[hbm, vm, hbm, hbm, hbm, hbm],
        out_specs=(hbm, vm),
        scratch_shapes=scratch,
        compiler_params=pltpu.CompilerParams(
            collective_id=0, has_side_effects=True, vmem_limit_bytes=60 * 1024 * 1024),
    )(tokens, routing[0].T, router_weight, w_gate, w_up, w_down)


def solution(mesh):
    placed = (
        P("seq", ("ctx", "exp"), None),
        P("seq", ("ctx", "exp"), None),
        P(),
        P(("seq", "exp"), None, "ctx"),
        P(("seq", "exp"), None, "ctx"),
        P(("seq", "exp"), "ctx", None),
    )
    return jax.shard_map(
        on_device,
        mesh=mesh,
        in_specs=placed,
        out_specs=(P("seq", ("ctx", "exp"), None), P("seq", None)),
        check_vma=False,
    )
```

```python
import functools

import jax
import jax.numpy as jnp
from jax import lax
from jax.experimental import pallas as pl
from jax.experimental.pallas import tpu as pltpu
from jax.sharding import PartitionSpec as P

route_scale = 2.5
LANES = 128
SUBS = 8
MESH = pl.DeviceIdType.MESH
f32 = jnp.float32
bf16 = jnp.bfloat16


def dot(a, b):
    return jnp.dot(a, b, preferred_element_type=f32)


def pack(rows, cap):
    sub = lax.broadcasted_iota(jnp.int32, (1, SUBS, LANES), 1)
    pieces = []
    for q in range(cap):
        piece = rows[:, :, q * LANES : (q + 1) * LANES]
        for s in range(cap, SUBS):
            piece = jnp.where(sub == s, rows[:, q : q + 1, s * LANES : (s + 1) * LANES], piece)
        pieces.append(piece)
    return jnp.concatenate(pieces, axis=2)


def unpack(dense, cap):
    sub = lax.broadcasted_iota(jnp.int32, (1, SUBS, LANES), 1)
    pieces = []
    for b in range(SUBS):
        if b < cap:
            piece = dense[:, :, b * LANES : (b + 1) * LANES]
        else:
            piece = jnp.broadcast_to(dense[:, b : b + 1, 0:LANES], dense.shape[:2] + (LANES,))
            for r in range(1, cap):
                piece = jnp.where(sub == r, dense[:, b : b + 1, r * LANES : (r + 1) * LANES], piece)
        pieces.append(piece)
    return jnp.concatenate(pieces, axis=2)


def kernel(
    cfg,
    tokens, routes_t, router_weight, w_gate, w_up, w_down,
    out, bal,
    tok, rw, wg, wu, wd, outv,
    mout, minn, xs, acc, logits, sel_s, gates, hid,
    ps, pr, keep, ys, yr, ykeep, rout, rin, stat,
    tok_sem, rw_sem, wg_sem, wu_sem, wd_sem, out_sem,
    d_send, d_recv, y_send, y_recv, c_send, c_recv,
    p_send, p_recv, v_send, v_recv, r_send, r_recv, s_send, s_recv,
):
    (steps, width, cap, flight, n_seq, n_ctx, n_exp, n_tok, top, experts) = cfg
    n_y = n_ctx // 2
    slots = flight * SUBS
    rows = flight * cap
    length = n_tok * n_ctx * n_exp
    seq, ctx, exp = lax.axis_index("seq"), lax.axis_index("ctx"), lax.axis_index("exp")
    me = seq * n_exp + exp
    my_y, core = ctx // 2, ctx % 2

    def group(o):
        p = (me + o) % flight
        return p, (p // n_exp, ctx, p % n_exp)

    def y_peer(o):
        y = (my_y + o) % n_y
        return y, (seq, y * 2 + core, exp)

    partner = (seq, ctx + 1 - 2 * core, exp)

    barrier = pltpu.get_barrier_semaphore()
    for o in range(1, flight):
        pl.semaphore_signal(barrier, inc=1, device_id=group(o)[1], device_id_type=MESH)
    for o in range(1, n_ctx):
        pl.semaphore_signal(barrier, inc=1, device_id=(seq, (ctx + o) % n_ctx, exp), device_id_type=MESH)

    def local(c, which):
        cols = pl.ds(pl.multiple_of(c * width, width), width)
        src, dst, sem = (
            lambda: (tokens.at[0, :, cols], tok.at[c], tok_sem.at[c]),
            lambda: (router_weight.at[cols], rw.at[c], rw_sem.at[c]),
            lambda: (w_gate.at[0, cols], wg.at[c], wg_sem.at[c]),
            lambda: (w_up.at[0, cols], wu.at[c], wu_sem.at[c]),
            lambda: (w_down.at[0, :, cols], wd.at[c], wd_sem.at[c]),
            lambda: (outv.at[c], out.at[0, :, cols], out_sem.at[c]),
        )[which]()
        return pltpu.make_async_copy(src, dst, sem)

    @pl.loop(0, steps)
    def _(c):
        local(c, 0).start()

    rt = routes_t[...]
    slot_expert = lax.broadcasted_iota(jnp.int32, (slots, n_tok), 0)
    hit_t = jnp.zeros((slots, n_tok), f32)
    for k in range(top):
        hit_t = hit_t + (rt[k : k + 1, :] == slot_expert // SUBS).astype(f32)
    ti = lax.broadcasted_iota(jnp.int32, (n_tok, n_tok), 0)
    tj = lax.broadcasted_iota(jnp.int32, (n_tok, n_tok), 1)
    rank_t = dot(hit_t.astype(bf16), (ti < tj).astype(f32).astype(bf16))
    pick_t = jnp.where(rank_t == (slot_expert % SUBS).astype(f32), hit_t, 0.0)
    sel_s[...] = pick_t.astype(bf16)

    def dispatch(c, o):
        p, dev = group(o)
        return pltpu.make_async_remote_copy(
            src_ref=mout.at[c, p], dst_ref=minn.at[c, me], send_sem=d_send.at[c, o], recv_sem=d_recv.at[c, o],
            device_id=dev, device_id_type=MESH)

    def spread(c, o):
        _, dev = y_peer(o)
        return pltpu.make_async_remote_copy(
            src_ref=xs.at[c, ctx], dst_ref=xs.at[c, ctx], send_sem=y_send.at[c, o], recv_sem=y_recv.at[c, o],
            device_id=dev, device_id_type=MESH)

    def hand(c, o):
        y = (my_y + o) % n_y
        slot = y * 2 + core
        return pltpu.make_async_remote_copy(
            src_ref=xs.at[c, slot], dst_ref=xs.at[c, slot], send_sem=c_send.at[c, o], recv_sem=c_recv.at[c, o],
            device_id=partner, device_id_type=MESH)

    pl.semaphore_wait(barrier, flight - 1 + n_ctx - 1)

    @pl.loop(0, steps)
    def _(c):
        local(c, 0).wait()
        picked = dot(sel_s[...], tok[c]).reshape(flight, SUBS, width)
        mout[c] = pack(picked, cap).astype(bf16)
        minn[c, me] = mout[c, me]
        for o in range(1, flight):
            dispatch(c, o).start()
        for which in range(1, 4):
            local(c, which).start()

    @pl.loop(0, steps)
    def _(c):
        local(c, 4).start()

    def stat_ctx(o):
        return pltpu.make_async_remote_copy(
            src_ref=stat.at[ctx], dst_ref=stat.at[ctx], send_sem=s_send.at[o], recv_sem=s_recv.at[o],
            device_id=(seq, (ctx + o) % n_ctx, exp), device_id_type=MESH)

    def stat_exp(o):
        slot = n_ctx + exp
        return pltpu.make_async_remote_copy(
            src_ref=stat.at[slot], dst_ref=stat.at[slot], send_sem=s_send.at[n_ctx + o],
            recv_sem=s_recv.at[n_ctx + o], device_id=(seq, ctx, (exp + o) % n_exp), device_id_type=MESH)

    def weigh():
        scores = jax.nn.sigmoid(logits[...])
        affinity = scores / jnp.sum(scores, axis=1, keepdims=True)
        spare = jnp.zeros((n_tok - top, n_tok), f32)
        rr = jnp.concatenate([routes_t[...].astype(f32), spare], axis=0).T
        lane = lax.broadcasted_iota(jnp.int32, (n_tok, experts), 1).astype(f32)
        hit = jnp.zeros((n_tok, experts), f32)
        for k in range(top):
            hit = hit + (rr[:, k : k + 1] == lane).astype(f32)
        gate = hit * scores / jnp.sum(hit * scores, axis=1, keepdims=True) * route_scale
        stat[ctx, 0:1] = jnp.sum(affinity, axis=0, keepdims=True)
        stat[ctx, 1:2] = jnp.sum(hit, axis=0, keepdims=True)
        for o in range(1, n_ctx):
            stat_ctx(o).start()
        rank = dot((ti > tj).astype(f32).astype(bf16), hit.astype(bf16))
        ei = lax.broadcasted_iota(jnp.int32, (experts, slots), 0)
        ej = lax.broadcasted_iota(jnp.int32, (experts, slots), 1)
        widen = (ei == ej // SUBS).astype(f32).astype(bf16)
        place = (lax.broadcasted_iota(jnp.int32, (n_tok, slots), 1) % SUBS).astype(f32)
        here = dot(rank.astype(bf16), widen) == place
        high = gate.astype(bf16)
        low = (gate - high.astype(f32)).astype(bf16)
        gates[0] = jnp.where(here, dot(high, widen), 0.0).astype(bf16)
        gates[1] = jnp.where(here, dot(low, widen), 0.0).astype(bf16)

    def share():
        for o in range(1, n_ctx):
            stat_ctx(o).wait_recv()
        ctx_total = stat[0]
        for j in range(1, n_ctx):
            ctx_total = ctx_total + stat[j]
        stat[n_ctx + exp] = ctx_total
        for o in range(1, n_exp):
            stat_exp(o).start()

    ri = lax.broadcasted_iota(jnp.int32, (rows, slots), 0)
    rj = lax.broadcasted_iota(jnp.int32, (rows, slots), 1)
    squeeze = ((ri // cap == rj // SUBS) & (ri % cap == rj % SUBS)).astype(f32).astype(bf16)
    si = lax.broadcasted_iota(jnp.int32, (slots, rows), 0)
    sj = lax.broadcasted_iota(jnp.int32, (slots, rows), 1)
    expand = ((sj // cap == si // SUBS) & (sj % cap == si % SUBS)).astype(f32).astype(bf16)

    acc[...] = jnp.zeros_like(acc)
    logits[...] = jnp.zeros_like(logits)
    lag_c, lag_d = 4, 5
    lag_f, lag_g, lag_h = 1, 3, 6

    @pl.loop(0, steps + lag_d)
    def _(i):
        @pl.when(i < steps)
        def _():
            c = i
            for o in range(1, flight):
                dispatch(c, o).wait_recv()
            loose = unpack(minn[c].astype(f32), cap).reshape(slots, width).astype(bf16)
            xs[c, ctx] = dot(squeeze, loose).astype(bf16)
            for o in range(1, n_y):
                spread(c, o).start()
            hand(c, 0).start()
            local(c, 1).wait()
            logits[...] += dot(tok[c], rw[c])

        @pl.when(i == steps)
        def _():
            weigh()

        @pl.when((i >= lag_c) & (i < steps + lag_c))
        def _():
            c = i - lag_c
            for o in range(1, n_y):
                spread(c, n_y - o).wait_recv()
                hand(c, o).start()

        @pl.when(i >= lag_d)
        def _():
            c = i - lag_d
            for o in range(n_y):
                hand(c, o).wait_recv()
            x = jnp.concatenate([xs[c, j].astype(f32) for j in range(n_ctx)], axis=0).astype(bf16)
            local(c, 2).wait()
            local(c, 3).wait()
            acc[0] += dot(x, wg[c])
            acc[1] += dot(x, wu[c])

    gv = acc[0]
    hid[...] = (gv / (1.0 + jnp.exp(-gv)) * acc[1]).astype(bf16)

    def pair(c):
        return pltpu.make_async_remote_copy(
            src_ref=ps.at[c], dst_ref=pr.at[c], send_sem=p_send.at[c], recv_sem=p_recv.at[c],
            device_id=partner, device_id_type=MESH)

    def back_y(c, o):
        y, dev = y_peer(o)
        return pltpu.make_async_remote_copy(
            src_ref=ys.at[c, o], dst_ref=yr.at[c, o], send_sem=v_send.at[c, o], recv_sem=v_recv.at[c, o],
            device_id=dev, device_id_type=MESH)

    def back(c, o):
        p, dev = group(o)
        return pltpu.make_async_remote_copy(
            src_ref=rout.at[c, p], dst_ref=rin.at[c, me], send_sem=r_send.at[c, o], recv_sem=r_recv.at[c, o],
            device_id=dev, device_id_type=MESH)

    @pl.loop(0, steps + lag_h)
    def _(i):
        @pl.when(i < steps)
        def _():
            c = i
            local(c, 4).wait()
            part = dot(hid[...], wd[c])
            for y in range(n_y):
                a = part[(2 * y) * rows : (2 * y + 1) * rows]
                b = part[(2 * y + 1) * rows : (2 * y + 2) * rows]
                ps[c, y] = jnp.where(core == 0, b, a).astype(bf16)
                keep[c, y] = jnp.where(core == 0, a, b).astype(bf16)
            pair(c).start()

        @pl.when((i >= lag_f) & (i < steps + lag_f))
        def _():
            c = i - lag_f
            pair(c).wait_recv()
            for o in range(n_y):
                y = (my_y + o) % n_y
                both = keep[c, y].astype(f32) + pr[c, y].astype(f32)
                if o == 0:
                    ykeep[c] = both
                else:
                    ys[c, o] = both.astype(bf16)
                    back_y(c, o).start()

        @pl.when(i == lag_h - 1)
        def _():
            share()

        @pl.when((i >= lag_g) & (i < steps + lag_g))
        def _():
            c = i - lag_g
            total = ykeep[c]
            for o in range(1, n_y):
                back_y(c, o).wait_recv()
                total = total + yr[c, o].astype(f32)
            spaced = dot(expand, total.astype(bf16)).reshape(flight, SUBS, width)
            rout[c] = pack(spaced, cap).astype(bf16)
            rin[c, me] = rout[c, me]
            for o in range(1, flight):
                back(c, o).start()

        @pl.when(i >= lag_h)
        def _():
            c = i - lag_h
            for o in range(1, flight):
                back(c, o).wait_recv()
            got = unpack(rin[c].astype(f32), cap).reshape(slots, width).astype(bf16)
            outv[c] = (dot(gates[0], got) + dot(gates[1], got)).astype(bf16)
            local(c, 5).start()

    for o in range(1, n_exp):
        stat_exp(o).wait_recv()
    total = stat[n_ctx]
    for j in range(1, n_exp):
        total = total + stat[n_ctx + j]
    bal[...] = total[1:2] * (experts / (top * length)) * (total[0:1] / length) * experts

    for o in range(1, n_ctx):
        stat_ctx(o).wait_send()
    for o in range(1, n_exp):
        stat_exp(o).wait_send()

    @pl.loop(0, steps)
    def _(c):
        for o in range(1, flight):
            dispatch(c, o).wait_send()
            back(c, o).wait_send()
        for o in range(1, n_y):
            spread(c, o).wait_send()
            back_y(c, o).wait_send()
        for o in range(n_y):
            hand(c, o).wait_send()
        pair(c).wait_send()
        local(c, 5).wait()


def on_device(tokens, routing, router_weight, w_gate, w_up, w_down):
    n_seq, n_ctx, n_exp = (lax.axis_size(a) for a in ("seq", "ctx", "exp"))
    _, n_tok, features = tokens.shape
    top = routing.shape[2]
    experts = router_weight.shape[1]
    ff = w_gate.shape[2]
    flight = n_seq * n_exp
    mean_load = n_tok * top // experts
    cap = mean_load + mean_load // 4
    width = SUBS * LANES
    steps = features // width
    n_y = n_ctx // 2
    rows = flight * cap
    slots = flight * SUBS
    cfg = (steps, width, cap, flight, n_seq, n_ctx, n_exp, n_tok, top, experts)
    V = pltpu.VMEM
    dma = pltpu.SemaphoreType.DMA
    dense = cap * LANES
    scratch = [
        V((steps, n_tok, width), bf16), V((steps, width, experts), bf16), V((steps, width, ff), bf16),
        V((steps, width, ff), bf16), V((steps, ff, width), bf16), V((steps, n_tok, width), bf16),
        V((steps, flight, SUBS, dense), bf16), V((steps, flight, SUBS, dense), bf16),
        V((steps, n_ctx, rows, width), bf16), V((2, n_ctx * rows, ff), f32), V((n_tok, experts), f32),
        V((slots, n_tok), bf16),
        V((2, n_tok, slots), bf16), V((n_ctx * rows, ff), bf16),
        V((steps, n_y, rows, width), bf16), V((steps, n_y, rows, width), bf16), V((steps, n_y, rows, width), bf16),
        V((steps, n_y, rows, width), bf16), V((steps, n_y, rows, width), bf16), V((steps, rows, width), f32),
        V((steps, flight, SUBS, dense), bf16), V((steps, flight, SUBS, dense), bf16),
        V((n_ctx + n_exp, 2, experts), f32),
    ]
    scratch += [dma((steps,)) for _ in range(6)]
    scratch += [dma((steps, flight)), dma((steps, flight)), dma((steps, n_y)), dma((steps, n_y)),
                dma((steps, n_y)), dma((steps, n_y)), dma((steps,)), dma((steps,)),
                dma((steps, n_y)), dma((steps, n_y)), dma((steps, flight)), dma((steps, flight)),
                dma((n_ctx + n_exp,)), dma((n_ctx + n_exp,))]
    hbm = pl.BlockSpec(memory_space=pl.ANY)
    vm = pl.BlockSpec(memory_space=pltpu.VMEM)
    return pl.pallas_call(
        functools.partial(kernel, cfg),
        out_shape=(jax.ShapeDtypeStruct(tokens.shape, bf16), jax.ShapeDtypeStruct((1, experts), f32)),
        in_specs=[hbm, vm, hbm, hbm, hbm, hbm],
        out_specs=(hbm, vm),
        scratch_shapes=scratch,
        compiler_params=pltpu.CompilerParams(
            collective_id=0, has_side_effects=True, vmem_limit_bytes=60 * 1024 * 1024),
    )(tokens, routing[0].T, router_weight, w_gate, w_up, w_down)


def solution(mesh):
    placed = (
        P("seq", ("ctx", "exp"), None),
        P("seq", ("ctx", "exp"), None),
        P(),
        P(("seq", "exp"), None, "ctx"),
        P(("seq", "exp"), None, "ctx"),
        P(("seq", "exp"), "ctx", None),
    )
    return jax.shard_map(
        on_device,
        mesh=mesh,
        in_specs=placed,
        out_specs=(P("seq", ("ctx", "exp"), None), P("seq", None)),
        check_vma=False,
    )
```
